256 devices in a mesh: bx: 16 (over x, y), by: 16 (over z, core).
Axes of the slice: x: 4, y: 4, z: 8, core: 2. Of those that a mesh axis runs over, the one named last changes fastest.
Arguments:
- forcing: float32 [2432, 4096], P('by', 'bx'), may hold values from -20 to 20
- guess: float32 [2432, 4096], P('by', 'bx'), may hold values from -3 to 3
- shift: float32 [2432, 4096], P('by', 'bx'), may hold values from 0.05 to 2
- ocean_mask: int32 [2432, 4096], P('by', 'bx'), may hold values 0 or 1
Outputs:
- solution_field: float32 [2432, 4096], P('by', 'bx')
- residual: float32 [2432, 4096], P('by', 'bx')
- residual_norm: float32 [], replicated
The draws below stay inside these ranges and needn't reach their ends.
All inputs are finite; a program needn't handle non-finite values. No bound on the sum of `ocean_mask` on one device may be relied on, other than what follows from the above.
Results may differ from the reference program's by a relative error of at most 0.00002.
Values sent between devices are 32-bit elements; how exact they have to be, the bound alone decides.
A program may use at most 64 MiB of HBM per device.

```python
import math
import jax
import jax.numpy as jnp
from jax import lax

ITERS = 4
NX = 4096
NY = 2432


def draw_forcing(key, part):
    rows = jnp.arange(NY, dtype=jnp.float32)
    rising = 1.0 + 2.0 * rows / max(NY - 1, 1)
    rough = jnp.clip(jax.random.normal(key, (NY, NX), jnp.float32), -6.0, 6.0)
    values = rough * rising[:, None]
    return jnp.clip(values, -20.0, 20.0)


def touch_ends(entries, own_key, smallest, top_value):
    index_at = [jax.random.randint(jax.random.fold_in(own_key, axis), (), 0, length) for axis, length in enumerate(entries.shape)]
    widest = entries.shape.index(max(entries.shape))
    neighbour = index_at[:widest] + [(index_at[widest] + 1) % entries.shape[widest]] + index_at[widest + 1:]
    return entries.at[tuple(index_at)].set(smallest).at[tuple(neighbour)].set(top_value)


def levels(stream_key, dims, cuts, least, top_value):
    def one(axis_at, parts):
        draws = jax.random.uniform(jax.random.fold_in(jax.random.fold_in(stream_key, 6), axis_at), (parts,), jnp.float32, least / len(cuts), top_value / len(cuts))
        return jnp.repeat(jnp.exp(draws), dims[axis_at] // parts).reshape((-1,) + (1,) * (len(dims) - axis_at - 1))

    level = one(*cuts[0])
    for cut in cuts[1:]:
        level = level * one(*cut)
    return level


def scatter_about(key, shape, scale, reach, cuts=(), kind=jnp.bfloat16):
    entries = scale * jax.random.normal(key, shape, jnp.float32)
    if cuts:
        entries = entries * levels(key, shape, cuts, -0.22, 0.18)
    return jnp.clip(entries, -reach, reach).astype(kind)


def setup_inputs(seed: int = 0) -> dict:
    streams_of = jax.random.split(jax.random.key(seed), 5)
    return {
        "forcing": draw_forcing(jax.random.fold_in(streams_of[4], 71), 0),
        "guess": scatter_about(streams_of[1], (NY, NX), 0.5, 3.0, ((0, 16), (1, 16)), jnp.float32),
        "shift": jnp.clip(jnp.exp(math.log(2.0) - 3.6888794 * jax.random.uniform(streams_of[2], (NY, NX), jnp.float32) ** levels(streams_of[2], (NY, NX), ((0, 16), (1, 16)), -0.2, 0.2)), 0.05, 2.0),
        "ocean_mask": touch_ends((jax.random.randint(streams_of[3], (NY, NX), 0, 5) < 4).astype(jnp.int32), jax.random.fold_in(streams_of[3], 1), 0, 1),
    }


LOW_BOUND = 0.05
HIGH_BOUND = 14.5

def extend(values):
    zonal = jnp.concatenate([values[:, -1:], values, values[:, :1]], axis=1)
    top_row = zonal[-1, ::-1]
    bottom_row = jnp.zeros_like(top_row)
    return jnp.concatenate([bottom_row[None, :], zonal, top_row[None, :]], axis=0)

def nine_point(values, shift, mask_f):
    padded = extend(values)
    center = padded[1:-1, 1:-1]
    sides = padded[2:, 1:-1] + padded[:-2, 1:-1] + padded[1:-1, 2:] + padded[1:-1, :-2]
    corners = padded[2:, 2:] + padded[2:, :-2] + padded[:-2, 2:] + padded[:-2, :-2]
    return mask_f * ((6.0 + shift) * center - sides - 0.5 * corners)

def pair_add(first, second):
    total = first[0] + second[0]
    backed = total - first[0]
    error = first[0] - (total - backed) + (second[0] - backed)
    error = error + first[1] + second[1]
    upper = total + error
    lower = error - (upper - total)
    return (upper, lower)

def tree_total(uppers, lowers):
    while uppers.shape[0] > 1:
        if uppers.shape[0] % 2 == 1:
            uppers = jnp.concatenate([uppers, jnp.zeros((1,), uppers.dtype)])
            lowers = jnp.concatenate([lowers, jnp.zeros((1,), lowers.dtype)])
        uppers, lowers = pair_add((uppers[0::2], lowers[0::2]), (uppers[1::2], lowers[1::2]))
    return (uppers[0], lowers[0])

def reference(forcing, guess, shift, ocean_mask):
    mask_f = ocean_mask.astype(jnp.float32)
    theta = (HIGH_BOUND + LOW_BOUND) / 2.0
    delta = (HIGH_BOUND - LOW_BOUND) / 2.0
    sigma = theta / delta
    rho = 1.0 / sigma
    iterate = mask_f * guess
    resid = mask_f * forcing - nine_point(iterate, shift, mask_f)
    direction = resid / theta
    for sweep in range(ITERS):
        iterate = iterate + direction
        resid = resid - nine_point(direction, shift, mask_f)
        rho_next = 1.0 / (2.0 * sigma - rho)
        direction = rho_next * rho * direction + 2.0 * rho_next / delta * resid
        rho = rho_next
    row_sums = lax.optimization_barrier(jnp.sum(resid * resid, axis=1))
    upper, lower = tree_total(row_sums, jnp.zeros_like(row_sums))
    norm_value = jnp.sqrt((upper + lower) / (NX * NY))
    return (iterate, resid, norm_value)
```

```python
import functools

import jax
import jax.numpy as jnp
from jax import lax
from jax.experimental import pallas as pl
from jax.experimental.pallas import tpu as pltpu
from jax.sharding import PartitionSpec as P

ITERS = 4
LOW_BOUND = 0.05
HIGH_BOUND = 14.5
MESH = pl.DeviceIdType.MESH
F32 = jnp.float32
L = 128
S = 8
F, X, C, M = range(4)


def pair_add(first, second):
    total = first[0] + second[0]
    backed = total - first[0]
    error = first[0] - (total - backed) + (second[0] - backed)
    error = error + first[1] + second[1]
    upper = total + error
    lower = error - (upper - total)
    return (upper, lower)


def tree_total(pairs):
    while len(pairs) > 1:
        odd = pairs[len(pairs) & ~1 :]
        pairs = [pair_add(a, b) for a, b in zip(pairs[0::2], pairs[1::2])] + odd
    return pairs[0]


def lanes(shape):
    return lax.broadcasted_iota(jnp.int32, shape, len(shape) - 1)


def smooth(tiles):
    lane = lanes(tiles[0].shape)
    left = [pltpu.roll(t, 1, 1) for t in tiles]
    right = [pltpu.roll(t, L - 1, 1) for t in tiles]
    n = len(tiles)
    out = []
    for k, t in enumerate(tiles):
        west = jnp.where(lane == 0, left[k - 1], left[k])
        east = jnp.where(lane == L - 1, right[(k + 1) % n], right[k])
        out.append(t + 0.5 * (west + east))
    return out


def reversed_tile(tile):
    lane = lanes(tile.shape)
    row = lax.broadcasted_iota(jnp.int32, tile.shape, 0)
    for bit in (1, 2, 4, 8, 16, 32, 64):
        tile = jnp.where(lane & bit != 0, pltpu.roll(tile, bit, 1), pltpu.roll(tile, L - bit, 1))
    for bit in (1, 2, 4):
        tile = jnp.where(row & bit != 0, pltpu.roll(tile, bit, 0), pltpu.roll(tile, S - bit, 0))
    return tile


def kernel(nbx, nby, f_hbm, g_hbm, s_hbm, m_hbm, x_hbm, r_hbm, norm_ref,
           e, mi, g, xo, ro, pack, fold, foldpack, colr, corn, ra, rb,
           in_sem, hs_sem, hr_sem, as_sem, ar_sem, bs_sem, br_sem, out_sem):
    bx, by = lax.axis_index("bx"), lax.axis_index("by")
    top = nby - 1
    rows = mi.shape[1]
    full = rows + 2 * S
    nt = rows // S
    nv = pack.shape[1]
    is_top, is_low = by == top, by == 0

    def dev(dx, dy):
        return (lax.rem(bx + dx + nbx, nbx), by + dy)

    loads = []
    for i, src in ((3, m_hbm), (1, g_hbm), (0, f_hbm), (2, s_hbm)):
        for t in range(2):
            dst = mi.at[t] if i == M else e.at[i, t, pl.ds(S, rows)]
            loads.append(pltpu.make_async_copy(src.at[:, pl.ds(L * t, L)], dst, in_sem.at[2 * i + t]))
            loads[-1].start()

    barrier = pltpu.get_barrier_semaphore()
    for o in range(1, nby):
        pl.semaphore_signal(barrier, 1, device_id=(bx, lax.rem(by + o, nby)), device_id_type=MESH)
    for o in range(1, nbx):
        pl.semaphore_signal(barrier, 1, device_id=(lax.rem(bx + o, nbx), by), device_id_type=MESH)
    for dy, there in ((1, by < top), (-1, by > 0)):
        @pl.when(there)
        def _():
            for dx in (1, -1):
                pl.semaphore_signal(barrier, 1, device_id=dev(dx, dy), device_id_type=MESH)

    zero_row = jnp.zeros((S, L), F32)
    for b in range(2):
        for t in range(3):
            g[b, t, 0:S] = zero_row
            g[b, t, pl.ds(S + full, S)] = zero_row

    @pl.when(is_low)
    def _():
        for i in range(4):
            for t in range(3):
                e[i, t, 0:S] = zero_row

    for c in loads:
        c.wait()
    for t in range(2):
        e[M, t, pl.ds(S, rows)] = mi[t].astype(F32)

    slot = lanes((S, L)) // 8
    for v in range(nv):
        for side in range(2):
            acc = zero_row
            for k in range(16):
                t, a = 4 * v + k // 4, k % 4
                if t < nt:
                    tile = e[a, 1 - side, pl.ds(S + S * t, S)]
                    acc = jnp.where(slot == k, pltpu.roll(tile, (8 * k + 8 * (1 - side)) % L, 1), acc)
            pack[side, v] = acc

    @pl.when(is_top)
    def _():
        for side in range(2):
            acc = zero_row
            for a in range(4):
                tile = reversed_tile(e[a, side, pl.ds(rows, S)])
                fold[a, 1 - side] = tile
                acc = jnp.where(slot == a, pltpu.roll(tile, (8 * a + 8 * (1 - side)) % L, 1), acc)
            foldpack[side] = acc

    pl.semaphore_wait(barrier, nbx + nby - 2 + jnp.where(is_top, 0, 2) + jnp.where(is_low, 0, 2))

    def remote(src, dst, sent, got, target):
        return pltpu.make_async_remote_copy(
            src_ref=src, dst_ref=dst, send_sem=hs_sem.at[sent], recv_sem=hr_sem.at[got],
            device_id=target, device_id_type=MESH)

    def strip(row):
        return e.at[:, pl.ds(0, 2), pl.ds(row, S)]

    last = nv - 1
    self_left = lax.rem(nbx - bx, nbx)
    self_right = lax.rem(2 * nbx - 2 - bx, nbx)
    not_top, not_low = by < top, by > 0
    fold_left = jnp.logical_and(is_top, self_left != bx)
    fold_right = jnp.logical_and(is_top, self_right != bx)
    sends = [
        (not_top, remote(pack.at[0, last], corn.at[0], 4, 4, dev(1, 1))),
        (not_top, remote(pack.at[1, last], corn.at[1], 5, 5, dev(-1, 1))),
        (not_low, remote(pack.at[0, 0], corn.at[2], 6, 6, dev(1, -1))),
        (not_low, remote(pack.at[1, 0], corn.at[3], 7, 7, dev(-1, -1))),
        (fold_left, remote(foldpack.at[0], corn.at[2], 8, 6, (self_left, by))),
        (fold_right, remote(foldpack.at[1], corn.at[3], 9, 7, (self_right, by))),
        (None, remote(pack.at[0], colr.at[0], 0, 0, dev(1, 0))),
        (None, remote(pack.at[1], colr.at[1], 1, 1, dev(-1, 0))),
        (not_top, remote(strip(rows), strip(0), 2, 2, dev(0, 1))),
        (is_top, remote(fold, strip(S + rows), 10, 3, (nbx - 1 - bx, by))),
        (not_low, remote(strip(S), strip(S + rows), 3, 3, dev(0, -1))),
    ]
    near = (bx, by)
    receipts = [
        (None, remote(pack.at[0], colr.at[0], 0, 0, near)),
        (None, remote(pack.at[1], colr.at[1], 1, 1, near)),
        (not_low, remote(strip(rows), strip(0), 2, 2, near)),
        (None, remote(strip(S), strip(S + rows), 3, 3, near)),
        (not_low, remote(pack.at[0, last], corn.at[0], 4, 4, near)),
        (not_low, remote(pack.at[1, last], corn.at[1], 5, 5, near)),
        (jnp.logical_or(not_top, fold_left), remote(pack.at[0, 0], corn.at[2], 6, 6, near)),
        (jnp.logical_or(not_top, fold_right), remote(pack.at[1, 0], corn.at[3], 7, 7, near)),
    ]

    def each(items, act):
        for cond, copy in items:
            if cond is None:
                act(copy)
            else:
                pl.when(cond)(functools.partial(act, copy))

    each(sends, lambda c: c.start())
    for k, (mine, target) in enumerate(((fold_left, self_left), (fold_right, self_right))):
        @pl.when(jnp.logical_and(is_top, target == bx))
        def _():
            corn[2 + k] = foldpack[k]

    @pl.when(is_low)
    def _():
        corn[0] = zero_row
        corn[1] = zero_row

    each(receipts, lambda c: c.wait_recv())
    each(sends, lambda c: c.wait_send())

    lane = lanes((S, L))
    for v in range(nv):
        for k in range(16):
            t, a = 4 * v + k // 4, k % 4
            if t < nt:
                e[a, 2, pl.ds(S + S * t, S)] = jnp.where(
                    lane < L // 2, pltpu.roll(colr[1, v], (L - 8 * k) % L, 1), pltpu.roll(colr[0, v], (2 * L - 8 - 8 * k) % L, 1))
    for side, (row, first) in enumerate(((0, 4 * ((nt - 1) % 4)), (S + rows, 0))):
        for a in range(4):
            k = first + a
            e[a, 2, pl.ds(row, S)] = jnp.where(
                lane < L // 2, pltpu.roll(corn[2 * side + 1], (L - 8 * k) % L, 1),
                pltpu.roll(corn[2 * side], (2 * L - 8 - 8 * k) % L, 1))

    theta = (HIGH_BOUND + LOW_BOUND) / 2.0
    delta = (HIGH_BOUND - LOW_BOUND) / 2.0
    sigma = theta / delta
    rho = 1.0 / sigma
    tall = 56
    blocks = [(a, min(tall, full - a)) for a in range(0, full, tall)]

    def own(a, n, value):
        lo, hi = max(a, S), min(a + n, S + rows)
        return pl.ds(lo - S, hi - lo), value[lo - a : hi - a]

    def add_up(a, n, tiles, fresh=None):
        for t in range(2):
            where, part = own(a, n, tiles[t])
            base = own(a, n, fresh[t])[1] if fresh else xo[where, pl.ds(L * t, L)]
            xo[where, pl.ds(L * t, L)] = base + part

    for a, n in blocks:
        at = pl.ds(a, n)
        v = [e[M, t, at] * e[X, t, at] for t in range(3)]
        for t, h in enumerate(smooth(v)):
            g[0, t, pl.ds(S + a, n)] = h
            e[X, t, at] = v[t]

    for sweep in range(ITERS):
        now, later = sweep % 2, 1 - sweep % 2
        rho_next = 1.0 / (2.0 * sigma - rho)
        for a, n in blocks:
            at = pl.ds(a, n)
            fresh = []
            for t in range(3):
                mid = g[now, t, pl.ds(S + a, n)]
                tall_sum = (mid + mid) + (g[now, t, pl.ds(S + a - 1, n)] + g[now, t, pl.ds(S + a + 1, n)])
                m, v = e[M, t, at], e[X, t, at]
                if sweep == 0:
                    c = m * (8.0 + e[C, t, at])
                    e[C, t, at] = c
                    r = m * e[F, t, at] - (c * v - m * tall_sum)
                    d = r * (1.0 / theta)
                    if t < 2:
                        where, base = own(a, n, v)
                        xo[where, pl.ds(L * t, L)] = base + own(a, n, d)[1]
                else:
                    r = e[F, t, at] - (e[C, t, at] * v - m * tall_sum)
                    d = (rho_next * rho) * v + (2.0 * rho_next / delta) * r
                    if t < 2:
                        where, part = own(a, n, d)
                        xo[where, pl.ds(L * t, L)] = xo[where, pl.ds(L * t, L)] + part
                e[F, t, at] = r
                e[X, t, at] = d
                fresh.append(d)
            for t, h in enumerate(smooth(fresh)):
                g[later, t, pl.ds(S + a, n)] = h
        if sweep > 0:
            rho = rho_next

    now = ITERS % 2
    x_out = pltpu.make_async_copy(xo, x_hbm, out_sem.at[0])
    x_out.start()
    sums = []
    for a in range(S, S + rows, 4 * S):
        n = min(4 * S, S + rows - a)
        at = pl.ds(a, n)
        squares = []
        for t in range(2):
            mid = g[now, t, pl.ds(S + a, n)]
            tall_sum = (mid + mid) + (g[now, t, pl.ds(S + a - 1, n)] + g[now, t, pl.ds(S + a + 1, n)])
            r = e[F, t, at] - (e[C, t, at] * e[X, t, at] - e[M, t, at] * tall_sum)
            ro[pl.ds(a - S, n), pl.ds(L * t, L)] = r
            squares.append(r * r)
        row_sums = jnp.broadcast_to(jnp.sum(squares[0] + squares[1], axis=1, keepdims=True), (n, L))
        sums += [row_sums[k : k + S] for k in range(0, n, S)]
    r_out = pltpu.make_async_copy(ro, r_hbm, out_sem.at[1])
    r_out.start()

    pair = tree_total([(q, jnp.zeros_like(q)) for q in sums])
    for bit in (4, 2, 1):
        pair = pair_add(pair, tuple(pltpu.roll(p, bit, 0) for p in pair))
    pair = tuple(p[0:1] for p in pair)

    sent = []
    for buf, me, n, ssem, rsem, target in (
        (ra, by, nby, as_sem, ar_sem, lambda p: (bx, p)),
        (rb, bx, nbx, bs_sem, br_sem, lambda p: (p, by)),
    ):
        buf[me, 0] = pair[0]
        buf[me, 1] = pair[1]
        for o in range(1, n):
            c = pltpu.make_async_remote_copy(
                src_ref=buf.at[me], dst_ref=buf.at[me], send_sem=ssem.at[o], recv_sem=rsem.at[me],
                device_id=target(lax.rem(me + o, n)), device_id_type=MESH)
            c.start()
            sent.append(c)
        for o in range(1, n):
            p = lax.rem(me + o, n)
            pltpu.make_async_remote_copy(
                src_ref=buf.at[p], dst_ref=buf.at[p], send_sem=ssem.at[o], recv_sem=rsem.at[p],
                device_id=target(p), device_id_type=MESH).wait_recv()
        pair = tree_total([(buf[p, 0], buf[p, 1]) for p in range(n)])

    cells = (rows * nby) * (2 * L * nbx)
    norm_ref[...] = jnp.sqrt((pair[0] + pair[1]) / float(cells))
    for c in sent:
        c.wait_send()
    x_out.wait()
    r_out.wait()


def solution(mesh):
    nbx, nby = mesh.shape["bx"], mesh.shape["by"]

    def step(forcing, guess, shift, ocean_mask):
        rows, cols = forcing.shape
        full, nt = rows + 2 * S, rows // S
        nv = -(-nt // 4)
        dma = pltpu.SemaphoreType.DMA
        x, r, norm = pl.pallas_call(
            functools.partial(kernel, nbx, nby),
            out_shape=(
                jax.ShapeDtypeStruct((rows, cols), F32),
                jax.ShapeDtypeStruct((rows, cols), F32),
                jax.ShapeDtypeStruct((1, L), F32),
            ),
            in_specs=[pl.BlockSpec(memory_space=pl.ANY)] * 4,
            out_specs=(
                pl.BlockSpec(memory_space=pl.ANY),
                pl.BlockSpec(memory_space=pl.ANY),
                pl.BlockSpec(memory_space=pltpu.VMEM),
            ),
            scratch_shapes=[
                pltpu.VMEM((4, 3, full, L), F32),
                pltpu.VMEM((2, rows, L), jnp.int32),
                pltpu.VMEM((2, 3, full + 2 * S, L), F32),
                pltpu.VMEM((rows, cols), F32),
                pltpu.VMEM((rows, cols), F32),
                pltpu.VMEM((2, nv, S, L), F32),
                pltpu.VMEM((4, 2, S, L), F32),
                pltpu.VMEM((2, S, L), F32),
                pltpu.VMEM((2, nv, S, L), F32),
                pltpu.VMEM((4, S, L), F32),
                pltpu.VMEM((nby, 2, 1, L), F32),
                pltpu.VMEM((nbx, 2, 1, L), F32),
                dma((8,)), dma((11,)), dma((8,)),
                dma((nby,)), dma((nby,)), dma((nbx,)), dma((nbx,)),
                dma((2,)),
            ],
            compiler_params=pltpu.CompilerParams(collective_id=0, has_side_effects=True),
        )(forcing, guess, shift, ocean_mask)
        return x, r, norm[0, 0]

    spec = P("by", "bx")
    return jax.shard_map(
        step, mesh=mesh, in_specs=(spec, spec, spec, spec), out_specs=(spec, spec, P()), check_vma=False
    )
```
